32 devices in a mesh: section: 2 (over core), row: 4 (over y, x), col: 4 (over z).
Axes of the slice: x: 2, y: 2, z: 4, core: 2. Of those that a mesh axis runs over, the one named last changes fastest.
Arguments:
- section_inputs: bfloat16 [2, 2, 48, 4096], P('section', None, 'col', 'row'), may hold values from -6 to 6
- out_grad: bfloat16 [2, 48, 4096], P(None, 'col', 'row'), may hold values from -6 to 6
- gate_weight: bfloat16 [2, 4096, 14336], P('section', 'row', 'col'), may hold values from -0.09375 to 0.09375
- up_weight: bfloat16 [2, 4096, 14336], P('section', 'row', 'col'), may hold values from -0.09375 to 0.09375
- down_weight: bfloat16 [2, 14336, 4096], P('section', 'col', 'row'), may hold values from -0.046875 to 0.046875
Outputs:
- input_grads: bfloat16 [2, 2, 48, 4096], P('section', None, 'col', 'row')
- grad_gate: float32 [2, 4096, 14336], P('section', 'row', 'col')
- grad_up: float32 [2, 4096, 14336], P('section', 'row', 'col')
- grad_down: float32 [2, 14336, 4096], P('section', 'col', 'row')
The draws below stay inside these ranges and needn't reach their ends.
All inputs are finite; a program needn't handle non-finite values.
Results may differ from the reference program's by a relative error of at most 0.025.
Values may be sent and summed in bfloat16 or wider, within the bound.
A program may use at most 192 MiB of HBM per device.

```python
import jax
import jax.numpy as jnp

D = 4096
FF = 14336
MICRO = 2
SECTIONS = 2
TOKENS = 48
N_ROW = 4


def level_of(own_key, shape, pieces, low, top_value):
    gain, own = 1.0, jax.random.fold_in(own_key, 6)
    for position, shards_of in pieces:
        steps = jnp.exp(jax.random.uniform(jax.random.fold_in(own, position), (shards_of,), jnp.float32, low / len(pieces), top_value / len(pieces)))
        gain = gain * jnp.repeat(steps, shape[position] // shards_of).reshape([-1 if axis == position else 1 for axis in range(len(shape))])
    return gain


def gaussian(own_key, extent, scale, most, cuts=(), dtype=jnp.bfloat16):
    result = scale * jax.random.normal(own_key, extent, jnp.float32)
    if cuts:
        result = result * level_of(own_key, extent, cuts, -0.22, 0.18)
    return jnp.clip(result, -most, most).astype(dtype)


def setup_inputs(seed: int = 0) -> dict:
    arg_keys = jax.random.split(jax.random.key(seed), 6)
    section_inputs = gaussian(arg_keys[0], (SECTIONS, MICRO, TOKENS, D), 1.0, 6.0, ((0, 2), (2, 4), (3, 4)))
    out_grad = gaussian(arg_keys[1], (MICRO, TOKENS, D), 1.0, 6.0, ((1, 4), (2, 4)))
    gate_weight = gaussian(arg_keys[2], (SECTIONS, D, FF), D ** -0.5, 0.09375, ((0, 2), (1, 4), (2, 4)))
    up_weight = gaussian(arg_keys[3], (SECTIONS, D, FF), D ** -0.5, 0.09375, ((0, 2), (1, 4), (2, 4)))
    down_weight = gaussian(arg_keys[4], (SECTIONS, FF, D), FF ** -0.5, 0.046875, ((0, 2), (1, 4), (2, 4)))
    return dict(section_inputs=section_inputs, out_grad=out_grad, gate_weight=gate_weight, up_weight=up_weight, down_weight=down_weight)


def blocked_sum(left, right):
    width = D // N_ROW
    total = jnp.zeros((left.shape[0], right.shape[1]), jnp.float32)
    for block in range(N_ROW):
        piece = jnp.dot(left[:, block * width:(block + 1) * width], right[block * width:(block + 1) * width],
                        preferred_element_type=jnp.float32).astype(jnp.bfloat16)
        total = total + piece.astype(jnp.float32)
    return total


def layer_backward(x_rows, dy_rows, w_gate, w_up, w_down):
    gate_sum = blocked_sum(x_rows, w_gate)
    up_sum = blocked_sum(x_rows, w_up)
    sigmoid_gate = jax.nn.sigmoid(gate_sum)
    activated = gate_sum * sigmoid_gate
    slope = sigmoid_gate * (1.0 + gate_sum * (1.0 - sigmoid_gate))
    hidden = (activated * up_sum).astype(jnp.bfloat16)
    hidden_grad = blocked_sum(dy_rows, w_down.T)
    gate_grad = (hidden_grad * up_sum * slope).astype(jnp.bfloat16)
    up_grad = (hidden_grad * activated).astype(jnp.bfloat16)
    branch = jnp.dot(gate_grad, w_gate.T, preferred_element_type=jnp.float32)
    branch = branch + jnp.dot(up_grad, w_up.T, preferred_element_type=jnp.float32)
    input_grad = (dy_rows.astype(jnp.float32) + branch).astype(jnp.bfloat16)
    gate_update = jnp.dot(x_rows.T, gate_grad, preferred_element_type=jnp.float32)
    up_update = jnp.dot(x_rows.T, up_grad, preferred_element_type=jnp.float32)
    down_update = jnp.dot(hidden.T, dy_rows, preferred_element_type=jnp.float32)
    return input_grad, gate_update, up_update, down_update


def reference(section_inputs, out_grad, gate_weight, up_weight, down_weight):
    carried = [out_grad[micro_index] for micro_index in range(MICRO)]
    input_list = []
    gate_list = []
    up_list = []
    down_list = []
    for section_number in reversed(range(SECTIONS)):
        gate_total = jnp.zeros((D, FF), jnp.float32)
        up_total = jnp.zeros((D, FF), jnp.float32)
        down_total = jnp.zeros((FF, D), jnp.float32)
        produced = []
        for micro_index in range(MICRO):
            input_grad, gate_update, up_update, down_update = layer_backward(
                section_inputs[section_number, micro_index], carried[micro_index],
                gate_weight[section_number], up_weight[section_number], down_weight[section_number])
            produced.append(input_grad)
            gate_total = gate_total + gate_update
            up_total = up_total + up_update
            down_total = down_total + down_update
        carried = produced
        input_list.insert(0, jnp.stack(produced))
        gate_list.insert(0, gate_total)
        up_list.insert(0, up_total)
        down_list.insert(0, down_total)
    return jnp.stack(input_list), jnp.stack(gate_list), jnp.stack(up_list), jnp.stack(down_list)
```

```python
import jax
import jax.numpy as jnp
from jax import lax
from jax.experimental import pallas as pl
from jax.experimental.pallas import tpu as pltpu
from jax.sharding import PartitionSpec as P

CONTRACT_ROWS = (((0,), (0,)), ((), ()))
CONTRACT_COLS = (((1,), (1,)), ((), ()))


def passed_along(block, axis, distance):
    devices = range(lax.axis_size(axis))
    route = [(i - distance, i) for i in devices if i - distance in devices]
    return lax.ppermute(block, axis, route)


def spread_panel(panel):
    return lax.all_gather(panel, "col", axis=0, tiled=True)


def row_partials(make_terms, keep_rows):
    return lax.psum_scatter(
        make_terms(jnp.int32(0), keep_rows * lax.axis_size("row")).astype(jnp.bfloat16),
        "row",
        scatter_dimension=0,
        tiled=True,
    ).astype(jnp.float32)


def layer_backward(x_local, dy_local, w_both, w_down):
    hidden_width = w_down.shape[0]
    x_whole = spread_panel(x_local)
    dy_whole = spread_panel(dy_local)
    keep_rows = x_whole.shape[0] // lax.axis_size("row")

    def forward_terms(first_row, row_count):
        return jnp.dot(x_whole, w_both, preferred_element_type=jnp.float32)

    def backward_terms(first_row, row_count):
        return lax.dot_general(dy_whole, w_down, CONTRACT_COLS, preferred_element_type=jnp.float32)

    both_sums = row_partials(forward_terms, keep_rows)
    hidden_grad = row_partials(backward_terms, keep_rows)
    gate_sum = both_sums[:, :hidden_width]
    up_sum = both_sums[:, hidden_width:]
    sigmoid_gate = jax.nn.sigmoid(gate_sum)
    activated = gate_sum * sigmoid_gate
    slope = sigmoid_gate * (1.0 + gate_sum * (1.0 - sigmoid_gate))
    hidden = (activated * up_sum).astype(jnp.bfloat16)
    gate_grad = (hidden_grad * up_sum * slope).astype(jnp.bfloat16)
    up_grad = (hidden_grad * activated).astype(jnp.bfloat16)
    packed = jnp.concatenate([hidden, gate_grad, up_grad], axis=1)
    gathered = lax.all_gather(packed, "row", axis=0, tiled=True)
    hidden_whole = gathered[:, :hidden_width]
    both_grads = gathered[:, hidden_width:]
    branch_sum = lax.psum_scatter(
        lax.dot_general(
            both_grads, w_both, CONTRACT_COLS, preferred_element_type=jnp.float32
        ).astype(jnp.bfloat16),
        "col",
        scatter_dimension=0,
        tiled=True,
    ).astype(jnp.float32)
    input_grad = (dy_local.astype(jnp.float32) + branch_sum).astype(jnp.bfloat16)
    down_update = lax.dot_general(
        hidden_whole, dy_whole, CONTRACT_ROWS, preferred_element_type=jnp.float32
    )
    both_update = lax.dot_general(
        x_whole, both_grads, CONTRACT_ROWS, preferred_element_type=jnp.float32
    )
    return (input_grad, both_update, down_update)


def shards(section_inputs, out_grad, gate_weight, up_weight, down_weight):
    section_id = lax.axis_index("section")
    last_section = lax.axis_size("section") - 1
    is_last = section_id == last_section
    panels = section_inputs[0]
    w_both = jnp.concatenate([gate_weight[0], up_weight[0]], axis=1)
    w_down = down_weight[0]
    hidden_width = w_down.shape[0]
    micro_count = panels.shape[0]
    both_total = jnp.zeros(w_both.shape, jnp.float32)
    down_total = jnp.zeros(w_down.shape, jnp.float32)
    merged_shape = (micro_count * panels.shape[1], panels.shape[2])
    x_local = panels.reshape(merged_shape)
    top_grads = out_grad.reshape(merged_shape)
    received = jnp.zeros(merged_shape, jnp.bfloat16)
    merged_results = received
    for step_index in range(last_section + 1):
        is_active = section_id == last_section - step_index
        dy_local = jnp.where(is_last, top_grads, received)
        input_grad, both_update, down_update = layer_backward(x_local, dy_local, w_both, w_down)
        merged_results = jnp.where(is_active, input_grad, merged_results)
        both_total = both_total + jnp.where(is_active, both_update, 0.0)
        down_total = down_total + jnp.where(is_active, down_update, 0.0)
        if step_index < last_section:
            received = passed_along(input_grad, "section", -1)
    results = merged_results.reshape(panels.shape)
    return (
        results[None],
        both_total[:, :hidden_width][None],
        both_total[:, hidden_width:][None],
        down_total[None],
    )


ORDER = pl.DeviceIdType.MESH


def remote(src, dst, send_sem, recv_sem, target):
    return pltpu.make_async_remote_copy(
        src_ref=src, dst_ref=dst, send_sem=send_sem, recv_sem=recv_sem, device_id=target, device_id_type=ORDER
    )


def relay_kernel(
    x_ref, top_ref, gate_ref, up_ref, down_ref,
    grad_out, x_out, dy_out, packed_out,
    w_gate, w_up, w_down, x_slots, dy_slots, part_send, part_recv, spread, gate_sum, up_sum,
    branch, branch_send, branch_recv, result,
    w_sem, x_send_sem, x_recv_sem, dy_send_sem, dy_recv_sem, part_send_sem, part_recv_sem,
    spread_send_sem, spread_recv_sem, branch_send_sem, branch_recv_sem, out_sem, go_sem,
):
    section = lax.axis_index("section")
    row = lax.axis_index("row")
    col = lax.axis_index("col")
    rows, width = part_send.shape[2], part_send.shape[3]
    group = x_slots.shape[1]
    is_top = section == 1
    is_bottom = section == 0

    def row_peer(d):
        hi, lo = row // 2, row % 2
        return ((hi + d // 2) % 2) * 2 + (lo + d % 2) % 2

    def ahead(d):
        return (col + d) % 4

    def behind(d):
        return (col + 4 - d) % 4

    def weight_copy(a, d):
        cols = pl.ds(pl.multiple_of(row_peer(d) * width, width), width)
        if a == 2:
            return pltpu.make_async_copy(down_ref.at[cols, :], w_down.at[d], w_sem.at[2, d])
        source, target = ((gate_ref, w_gate), (up_ref, w_up))[a]
        return pltpu.make_async_copy(source.at[:, cols], target.at[d], w_sem.at[a, d])

    def x_copy(d):
        return remote(x_ref, x_slots.at[d], x_send_sem.at[d], x_recv_sem.at[d], (section, row, ahead(d)))

    def dy_copy(d):
        return remote(top_ref, dy_slots.at[d], dy_send_sem.at[d], dy_recv_sem.at[d], (section, row, ahead(d)))

    def pass_copy(d):
        return remote(result, dy_slots.at[d], dy_send_sem.at[d], dy_recv_sem.at[d], (0, row, ahead(d)))

    def part_copy(a, d):
        return remote(
            part_send.at[a, d], part_recv.at[a, d], part_send_sem.at[a, d], part_recv_sem.at[a, d],
            (section, row_peer(d), col),
        )

    def spread_copy(a, d):
        return remote(
            spread.at[a, 0], spread.at[a, d], spread_send_sem.at[a, d], spread_recv_sem.at[a, d],
            (section, row_peer(d), col),
        )

    def branch_copy(d):
        return remote(
            branch_send.at[d], branch_recv.at[d], branch_send_sem.at[d], branch_recv_sem.at[d],
            (section, row, behind(d)),
        )

    def merge(slots, whole):
        for d in range(4):
            branch[d * group:(d + 1) * group, :] = slots[d].astype(jnp.float32)
        whole[...] = branch[...].astype(jnp.bfloat16)

    for d in (1, 2, 3):
        x_copy(d).start()
    x_slots[0] = x_ref[...]

    @pl.when(is_top)
    def _():
        for d in (1, 2, 3):
            dy_copy(d).start()
        dy_slots[0] = top_ref[...]
        for d in (3, 2, 1, 0):
            weight_copy(2, d).start()

    for d in (3, 2, 1, 0):
        weight_copy(0, d).start()
        weight_copy(1, d).start()

    @pl.when(is_bottom)
    def _():
        for d in (3, 2, 1, 0):
            weight_copy(2, d).start()

    def hidden_terms():
        merge(dy_slots, dy_out)

        def step(i, carry):
            d = 3 - i
            weight_copy(2, d).wait()
            part_send[2, d] = lax.dot_general(
                dy_out[...], w_down[d], CONTRACT_COLS, preferred_element_type=jnp.float32
            ).astype(jnp.bfloat16)

            @pl.when(d > 0)
            def _():
                part_copy(2, d).start()
            return carry

        lax.fori_loop(0, 4, step, 0)

    @pl.when(is_top)
    def _():
        for d in (1, 2, 3):
            dy_copy(d).wait_recv()
        hidden_terms()

    for d in (1, 2, 3):
        x_copy(d).wait_recv()
    merge(x_slots, x_out)

    def forward_step(i, carry):
        d = 3 - i
        weight_copy(0, d).wait()
        weight_copy(1, d).wait()
        for a, weight in enumerate((w_gate, w_up)):
            part_send[a, d] = jnp.dot(
                x_out[...], weight[d], preferred_element_type=jnp.float32
            ).astype(jnp.bfloat16)

            @pl.when(jnp.logical_and(is_top, d > 0))
            def _():
                part_copy(a, d).start()
        return carry

    lax.fori_loop(0, 4, forward_step, 0)

    @pl.when(is_bottom)
    def _():
        pl.semaphore_wait(go_sem, 1)
        for d in (3, 2, 1):
            for a in range(2):
                part_copy(a, d).start()

    def summed(a, span):
        total = part_send[a, 0, span, :].astype(jnp.float32)
        for d in (1, 2, 3):
            total = total + part_recv[a, d, span, :].astype(jnp.float32)
        return total

    def span_of(i):
        return pl.ds(pl.multiple_of(i * 16, 16), 16)

    for a in range(2):
        for d in (1, 2, 3):
            part_copy(a, d).wait_recv()

    def hidden_step(i, carry):
        span = span_of(i)
        gate, up = summed(0, span), summed(1, span)
        gate_sum[span, :] = gate
        up_sum[span, :] = up
        spread[0, 0, span, :] = (gate * jax.nn.sigmoid(gate) * up).astype(jnp.bfloat16)
        return carry

    lax.fori_loop(0, rows // 16, hidden_step, 0)

    @pl.when(is_bottom)
    def _():
        for d in (3, 2, 1):
            spread_copy(0, d).start()
        for d in range(4):
            pass_copy(d).wait_recv()
        hidden_terms()

    for d in (1, 2, 3):
        part_copy(2, d).wait_recv()

    def grad_step(i, carry):
        span = span_of(i)
        hidden_grad = summed(2, span)
        gate, up = gate_sum[span, :], up_sum[span, :]
        sigmoid_gate = jax.nn.sigmoid(gate)
        slope = sigmoid_gate * (1.0 + gate * (1.0 - sigmoid_gate))
        spread[1, 0, span, :] = (hidden_grad * up * slope).astype(jnp.bfloat16)
        spread[2, 0, span, :] = (hidden_grad * (gate * sigmoid_gate)).astype(jnp.bfloat16)
        return carry

    lax.fori_loop(0, rows // 16, grad_step, 0)
    for d in (3, 2, 1):
        for a in (1, 2):
            spread_copy(a, d).start()

    branch[...] = jnp.zeros_like(branch)

    def branch_step(d, carry):
        @pl.when(d > 0)
        def _():
            spread_copy(1, d).wait_recv()
            spread_copy(2, d).wait_recv()

        branch[...] += lax.dot_general(
            spread[1, d], w_gate[d], CONTRACT_COLS, preferred_element_type=jnp.float32
        ) + lax.dot_general(
            spread[2, d], w_up[d], CONTRACT_COLS, preferred_element_type=jnp.float32
        )
        return carry

    lax.fori_loop(0, 4, branch_step, 0)
    for d in (3, 2, 1, 0):
        branch_send[d] = branch[d * group:(d + 1) * group, :].astype(jnp.bfloat16)
        if d:
            branch_copy(d).start()

    @pl.when(is_top)
    def _():
        pl.semaphore_signal(go_sem, inc=1, device_id=(0, row, col), device_id_type=ORDER)
        for d in (3, 2, 1):
            spread_copy(0, d).start()

    total = branch_send[0].astype(jnp.float32)
    for d in (1, 2, 3):
        branch_copy(d).wait_recv()
        total = total + branch_recv[d].astype(jnp.float32)
    result[...] = (dy_slots[0].astype(jnp.float32) + total).astype(jnp.bfloat16)

    @pl.when(is_top)
    def _():
        for d in (3, 2, 1, 0):
            pass_copy(d).start()

    grad_out[...] = result[...]
    for d in (1, 2, 3):
        spread_copy(0, d).wait_recv()

    def store_copy(a, d):
        cols = pl.ds(pl.multiple_of(row_peer(d) * width, width), width)
        return pltpu.make_async_copy(spread.at[a, d], packed_out.at[a, :, cols], out_sem.at[a, d])

    for a in range(3):
        for d in range(4):
            store_copy(a, d).start()
    for a in range(3):
        for d in range(4):
            store_copy(a, d).wait()
    for d in (1, 2, 3):
        x_copy(d).wait_send()
        branch_copy(d).wait_send()
        for a in range(3):
            part_copy(a, d).wait_send()
            spread_copy(a, d).wait_send()

    @pl.when(is_top)
    def _():
        for d in (1, 2, 3):
            dy_copy(d).wait_send()
        for d in range(4):
            pass_copy(d).wait_send()


def fast_shards(section_inputs, out_grad, gate_weight, up_weight, down_weight):
    panels = section_inputs[0]
    micro, local, width = panels.shape
    group = micro * local
    rows = group * lax.axis_size("col")
    hidden_width = gate_weight.shape[2]
    piece = hidden_width // lax.axis_size("row")
    vmem = pl.BlockSpec(memory_space=pltpu.VMEM)
    anywhere = pl.BlockSpec(memory_space=pl.ANY)
    bf16, f32 = jnp.bfloat16, jnp.float32
    dma = pltpu.SemaphoreType.DMA
    grad, x_whole, dy_whole, packed = pl.pallas_call(
        relay_kernel,
        out_shape=(
            jax.ShapeDtypeStruct((group, width), bf16),
            jax.ShapeDtypeStruct((rows, width), bf16),
            jax.ShapeDtypeStruct((rows, width), bf16),
            jax.ShapeDtypeStruct((3, rows, hidden_width), bf16),
        ),
        in_specs=[vmem, vmem, anywhere, anywhere, anywhere],
        out_specs=(vmem, vmem, vmem, anywhere),
        scratch_shapes=[
            pltpu.VMEM((4, width, piece), bf16),
            pltpu.VMEM((4, width, piece), bf16),
            pltpu.VMEM((4, piece, width), bf16),
            pltpu.VMEM((4, group, width), bf16),
            pltpu.VMEM((4, group, width), bf16),
            pltpu.VMEM((3, 4, rows, piece), bf16),
            pltpu.VMEM((3, 4, rows, piece), bf16),
            pltpu.VMEM((3, 4, rows, piece), bf16),
            pltpu.VMEM((rows, piece), f32),
            pltpu.VMEM((rows, piece), f32),
            pltpu.VMEM((rows, width), f32),
            pltpu.VMEM((4, group, width), bf16),
            pltpu.VMEM((4, group, width), bf16),
            pltpu.VMEM((group, width), bf16),
            dma((3, 4)), dma((4,)), dma((4,)), dma((4,)), dma((4,)),
            dma((3, 4)), dma((3, 4)), dma((3, 4)), dma((3, 4)), dma((4,)), dma((4,)),
            dma((3, 4)), pltpu.SemaphoreType.REGULAR,
        ],
        compiler_params=pltpu.CompilerParams(has_side_effects=True, vmem_limit_bytes=56 * 2**20),
    )(
        panels.reshape(group, width), out_grad.reshape(group, width),
        gate_weight[0], up_weight[0], down_weight[0],
    )
    grads = [
        lax.dot_general(left, right, CONTRACT_ROWS, preferred_element_type=f32)
        for left, right in ((x_whole, packed[1]), (x_whole, packed[2]), (packed[0], dy_whole))
    ]
    return (grad.reshape(panels.shape)[None], *(g[None] for g in grads))


def fits_kernel(mesh, gate_weight, section_inputs):
    sizes = mesh.shape
    if (sizes["section"], sizes["row"], sizes["col"]) != (2, 4, 4):
        return False
    piece = gate_weight.shape[2] // (sizes["row"] * sizes["col"])
    local = section_inputs.shape[1] * section_inputs.shape[2] // sizes["col"]
    return piece % 128 == 0 and local % 8 == 0 and (local * sizes["col"]) % 16 == 0


def solution(mesh):
    specs = dict(
        mesh=mesh,
        in_specs=(
            P("section", None, "col", "row"),
            P(None, "col", "row"),
            P("section", "row", "col"),
            P("section", "row", "col"),
            P("section", "col", "row"),
        ),
        out_specs=(
            P("section", None, "col", "row"),
            P("section", "row", "col"),
            P("section", "row", "col"),
            P("section", "col", "row"),
        ),
        check_vma=False,
    )

    def run(section_inputs, out_grad, gate_weight, up_weight, down_weight):
        body = fast_shards if fits_kernel(mesh, gate_weight, section_inputs) else shards
        return jax.shard_map(body, **specs)(section_inputs, out_grad, gate_weight, up_weight, down_weight)

    return run
```

```python
import jax
import jax.numpy as jnp
from jax import lax
from jax.experimental import pallas as pl
from jax.experimental.pallas import tpu as pltpu
from jax.sharding import PartitionSpec as P

CONTRACT_ROWS = (((0,), (0,)), ((), ()))
CONTRACT_COLS = (((1,), (1,)), ((), ()))


def passed_along(block, axis, distance):
    devices = range(lax.axis_size(axis))
    route = [(i - distance, i) for i in devices if i - distance in devices]
    return lax.ppermute(block, axis, route)


def spread_panel(panel):
    return lax.all_gather(panel, "col", axis=0, tiled=True)


def row_partials(make_terms, keep_rows):
    return lax.psum_scatter(
        make_terms(jnp.int32(0), keep_rows * lax.axis_size("row")).astype(jnp.bfloat16),
        "row",
        scatter_dimension=0,
        tiled=True,
    ).astype(jnp.float32)


def layer_backward(x_local, dy_local, w_both, w_down):
    hidden_width = w_down.shape[0]
    x_whole = spread_panel(x_local)
    dy_whole = spread_panel(dy_local)
    keep_rows = x_whole.shape[0] // lax.axis_size("row")

    def forward_terms(first_row, row_count):
        return jnp.dot(x_whole, w_both, preferred_element_type=jnp.float32)

    def backward_terms(first_row, row_count):
        return lax.dot_general(dy_whole, w_down, CONTRACT_COLS, preferred_element_type=jnp.float32)

    both_sums = row_partials(forward_terms, keep_rows)
    hidden_grad = row_partials(backward_terms, keep_rows)
    gate_sum = both_sums[:, :hidden_width]
    up_sum = both_sums[:, hidden_width:]
    sigmoid_gate = jax.nn.sigmoid(gate_sum)
    activated = gate_sum * sigmoid_gate
    slope = sigmoid_gate * (1.0 + gate_sum * (1.0 - sigmoid_gate))
    hidden = (activated * up_sum).astype(jnp.bfloat16)
    gate_grad = (hidden_grad * up_sum * slope).astype(jnp.bfloat16)
    up_grad = (hidden_grad * activated).astype(jnp.bfloat16)
    packed = jnp.concatenate([hidden, gate_grad, up_grad], axis=1)
    gathered = lax.all_gather(packed, "row", axis=0, tiled=True)
    hidden_whole = gathered[:, :hidden_width]
    both_grads = gathered[:, hidden_width:]
    branch_sum = lax.psum_scatter(
        lax.dot_general(
            both_grads, w_both, CONTRACT_COLS, preferred_element_type=jnp.float32
        ).astype(jnp.bfloat16),
        "col",
        scatter_dimension=0,
        tiled=True,
    ).astype(jnp.float32)
    input_grad = (dy_local.astype(jnp.float32) + branch_sum).astype(jnp.bfloat16)
    down_update = lax.dot_general(
        hidden_whole, dy_whole, CONTRACT_ROWS, preferred_element_type=jnp.float32
    )
    both_update = lax.dot_general(
        x_whole, both_grads, CONTRACT_ROWS, preferred_element_type=jnp.float32
    )
    return (input_grad, both_update, down_update)


def shards(section_inputs, out_grad, gate_weight, up_weight, down_weight):
    section_id = lax.axis_index("section")
    last_section = lax.axis_size("section") - 1
    is_last = section_id == last_section
    panels = section_inputs[0]
    w_both = jnp.concatenate([gate_weight[0], up_weight[0]], axis=1)
    w_down = down_weight[0]
    hidden_width = w_down.shape[0]
    micro_count = panels.shape[0]
    both_total = jnp.zeros(w_both.shape, jnp.float32)
    down_total = jnp.zeros(w_down.shape, jnp.float32)
    merged_shape = (micro_count * panels.shape[1], panels.shape[2])
    x_local = panels.reshape(merged_shape)
    top_grads = out_grad.reshape(merged_shape)
    received = jnp.zeros(merged_shape, jnp.bfloat16)
    merged_results = received
    for step_index in range(last_section + 1):
        is_active = section_id == last_section - step_index
        dy_local = jnp.where(is_last, top_grads, received)
        input_grad, both_update, down_update = layer_backward(x_local, dy_local, w_both, w_down)
        merged_results = jnp.where(is_active, input_grad, merged_results)
        both_total = both_total + jnp.where(is_active, both_update, 0.0)
        down_total = down_total + jnp.where(is_active, down_update, 0.0)
        if step_index < last_section:
            received = passed_along(input_grad, "section", -1)
    results = merged_results.reshape(panels.shape)
    return (
        results[None],
        both_total[:, :hidden_width][None],
        both_total[:, hidden_width:][None],
        down_total[None],
    )


ORDER = pl.DeviceIdType.MESH


def remote(src, dst, send_sem, recv_sem, target):
    return pltpu.make_async_remote_copy(
        src_ref=src, dst_ref=dst, send_sem=send_sem, recv_sem=recv_sem, device_id=target, device_id_type=ORDER
    )


def relay_kernel(
    x_ref, top_ref, gate_ref, up_ref, down_ref,
    grad_out, x_out, dy_out, packed_out,
    w_gate, w_up, w_down, x_slots, dy_slots, part_send, part_recv, spread, gate_sum, up_sum,
    branch, branch_send, branch_recv, result,
    w_sem, x_send_sem, x_recv_sem, dy_send_sem, dy_recv_sem, part_send_sem, part_recv_sem,
    spread_send_sem, spread_recv_sem, branch_send_sem, branch_recv_sem, onward_send_sem, onward_recv_sem, out_sem, go_sem,
):
    section = lax.axis_index("section")
    row = lax.axis_index("row")
    col = lax.axis_index("col")
    rows, width = part_send.shape[2], part_send.shape[3]
    local, micro = x_slots.shape[1:3]
    group = local * micro
    is_top = section == 1
    is_bottom = section == 0

    def row_peer(d):
        hi, lo = row // 2, row % 2
        return ((hi + d // 2) % 2) * 2 + (lo + d % 2) % 2

    def ahead(d):
        return (col + d) % 4

    def behind(d):
        return (col + 4 - d) % 4

    def weight_copy(a, d):
        cols = pl.ds(pl.multiple_of(row_peer(d) * width, width), width)
        if a == 2:
            return pltpu.make_async_copy(down_ref.at[cols, :], w_down.at[d], w_sem.at[2, d])
        source, target = ((gate_ref, w_gate), (up_ref, w_up))[a]
        return pltpu.make_async_copy(source.at[:, cols], target.at[d], w_sem.at[a, d])

    def x_copy(d):
        return remote(x_ref, x_slots.at[d], x_send_sem.at[d], x_recv_sem.at[d], (section, row, ahead(d)))

    def dy_copy(d):
        return remote(top_ref, dy_slots.at[d], dy_send_sem.at[d], dy_recv_sem.at[d], (section, row, ahead(d)))

    def pass_copy(d):
        return remote(result, dy_slots.at[d], dy_send_sem.at[d], dy_recv_sem.at[d], (0, row, ahead(d)))

    def half(h):
        return pl.ds(h * (rows // 2), rows // 2)

    def part_copy(a, d, h):
        return remote(
            part_send.at[a, d, half(h), :], part_recv.at[a, d, half(h), :],
            part_send_sem.at[a, d, h], part_recv_sem.at[a, d, h], (section, row_peer(d), col),
        )

    def spread_copy(a, d, h):
        return remote(
            spread.at[a, 0, half(h), :], spread.at[a, d, half(h), :],
            spread_send_sem.at[a, d, h], spread_recv_sem.at[a, d, h], (section, row_peer(d), col),
        )

    def onward_copy(a, d):
        return remote(
            spread.at[a, d, half(d - 1), :], spread.at[a, 3, half(d - 1), :],
            onward_send_sem.at[a, d], onward_recv_sem.at[a, d], (section, row_peer(3 - d), col),
        )

    def relay(*arrays):
        for d in (1, 2):
            for a in arrays:
                spread_copy(a, d, d - 1).wait_recv()
                onward_copy(a, d).start()
        for d in (1, 2):
            for a in arrays:
                spread_copy(a, d, 2 - d).wait_recv()

    def branch_copy(d):
        return remote(
            branch_send.at[d], branch_recv.at[d], branch_send_sem.at[d], branch_recv_sem.at[d],
            (section, row, behind(d)),
        )

    def merge(slots, whole):
        for d in range(4):
            for t in range(local):
                first = d * group + t * micro
                branch[first:first + micro, :] = slots[d, t].astype(jnp.float32)
        whole[...] = branch[...].astype(jnp.bfloat16)

    for d in (3, 2, 1, 0):
        weight_copy(0, d).start()
        weight_copy(1, d).start()
    for d in (3, 2, 1, 0):
        weight_copy(2, d).start()

    barrier = pltpu.get_barrier_semaphore()
    greeted = [(section, row, ahead(d)) for d in (1, 2, 3)]
    greeted += [(section, row_peer(d), col) for d in (1, 2, 3)]
    greeted += [(1 - section, row, ahead(d)) for d in range(4)]
    for device in greeted:
        pl.semaphore_signal(barrier, inc=1, device_id=device, device_id_type=ORDER)
    pl.semaphore_wait(barrier, len(greeted))

    for d in (2, 1, 3):
        x_copy(d).start()
    x_slots[0] = x_ref[...]

    @pl.when(is_top)
    def _():
        for d in (2, 1, 3):
            dy_copy(d).start()
        dy_slots[0] = top_ref[...]

    def hidden_terms():
        merge(dy_slots, dy_out)

        def step(i, carry):
            d = 3 - i
            weight_copy(2, d).wait()
            part_send[2, d] = lax.dot_general(
                dy_out[...], w_down[d], CONTRACT_COLS, preferred_element_type=jnp.float32
            ).astype(jnp.bfloat16)

            @pl.when(d > 0)
            def _():
                part_copy(2, d, 0).start()
            return carry

        lax.fori_loop(0, 4, step, 0)

    for d in (1, 2, 3):
        x_copy(d).wait_recv()
    merge(x_slots, x_out)

    def forward_step(i, carry):
        d = 3 - i
        weight_copy(0, d).wait()
        weight_copy(1, d).wait()
        for a, weight in enumerate((w_gate, w_up)):
            part_send[a, d] = jnp.dot(
                x_out[...], weight[d], preferred_element_type=jnp.float32
            ).astype(jnp.bfloat16)

            @pl.when(jnp.logical_and(is_top, d > 0))
            def _():
                part_copy(a, d, 0).start()
        return carry

    lax.fori_loop(0, 4, forward_step, 0)

    @pl.when(is_bottom)
    def _():
        pl.semaphore_wait(go_sem, 1)
        for h in range(2):
            for d in (3, 2, 1):
                for a in range(2):
                    part_copy(a, d, h).start()
        for d in range(4):
            pass_copy(d).wait_recv()

    @pl.when(is_top)
    def _():
        for d in (1, 2, 3):
            dy_copy(d).wait_recv()

    hidden_terms()

    @pl.when(is_top)
    def _():
        for d in (3, 2, 1):
            for a in range(2):
                part_copy(a, d, 1).start()

    for d in (3, 2, 1):
        part_copy(2, d, 1).start()

    def summed(a, span):
        total = part_send[a, 0, span, :].astype(jnp.float32)
        for d in (1, 2, 3):
            total = total + part_recv[a, d, span, :].astype(jnp.float32)
        return total

    def span_of(i):
        return pl.ds(pl.multiple_of(i * 16, 16), 16)

    def hidden_step(i, carry):
        span = span_of(i)
        gate, up = summed(0, span), summed(1, span)
        gate_sum[span, :] = gate
        up_sum[span, :] = up
        spread[0, 0, span, :] = (gate * jax.nn.sigmoid(gate) * up).astype(jnp.bfloat16)
        return carry

    def grad_step(i, carry):
        span = span_of(i)
        hidden_grad = summed(2, span)
        gate, up = gate_sum[span, :], up_sum[span, :]
        sigmoid_gate = jax.nn.sigmoid(gate)
        slope = sigmoid_gate * (1.0 + gate * (1.0 - sigmoid_gate))
        spread[1, 0, span, :] = (hidden_grad * up * slope).astype(jnp.bfloat16)
        spread[2, 0, span, :] = (hidden_grad * (gate * sigmoid_gate)).astype(jnp.bfloat16)
        return carry

    steps = rows // 32
    for h in range(2):
        for a in range(2):
            for d in (1, 2, 3):
                part_copy(a, d, h).wait_recv()
        lax.fori_loop(h * steps, (h + 1) * steps, hidden_step, 0)
        for d in (1, 2, 3):
            part_copy(2, d, h).wait_recv()
        lax.fori_loop(h * steps, (h + 1) * steps, grad_step, 0)
        for a in (1, 2):
            for d in (1, 2):
                spread_copy(a, d, h).start()

    @pl.when(is_bottom)
    def _():
        for h in range(2):
            for d in (1, 2):
                spread_copy(0, d, h).start()

    def partner_go():
        pl.semaphore_signal(go_sem, inc=1, device_id=(1 - section, row, col), device_id_type=ORDER)

    branch[...] = jnp.zeros_like(branch)

    def branch_step(d, carry):
        @pl.when(d == 1)
        def _():
            relay(1, 2)

        @pl.when(d == 3)
        def _():
            for a in (1, 2):
                for e in (1, 2):
                    onward_copy(a, e).wait_recv()
            partner_go()

        branch[...] += lax.dot_general(
            spread[1, d], w_gate[d], CONTRACT_COLS, preferred_element_type=jnp.float32
        ) + lax.dot_general(
            spread[2, d], w_up[d], CONTRACT_COLS, preferred_element_type=jnp.float32
        )
        return carry

    lax.fori_loop(0, 4, branch_step, 0)
    for d in (2, 3, 1, 0):
        branch_send[d] = branch[d * group:(d + 1) * group, :].astype(jnp.bfloat16)
        if d:
            branch_copy(d).start()

    def store_copy(a, d):
        cols = pl.ds(pl.multiple_of(row_peer(d) * width, width), width)
        return pltpu.make_async_copy(spread.at[a, d], packed_out.at[a, :, cols], out_sem.at[a, d])

    for a in (1, 2):
        for d in range(4):
            store_copy(a, d).start()

    total = dy_out[:group, :].astype(jnp.float32) + branch_send[0].astype(jnp.float32)
    for d in (1, 2, 3):
        branch_copy(d).wait_recv()
        total = total + branch_recv[d].astype(jnp.float32)
    branch[:group, :] = total
    for t in range(local):
        result[t] = branch[t * micro:(t + 1) * micro, :].astype(jnp.bfloat16)

    @pl.when(is_top)
    def _():
        for d in (2, 1, 3, 0):
            pass_copy(d).start()
        pl.semaphore_wait(go_sem, 1)
        for h in range(2):
            for d in (1, 2):
                spread_copy(0, d, h).start()

    grad_out[...] = result[...]
    relay(0)
    for d in (1, 2):
        onward_copy(0, d).wait_recv()
    for d in range(4):
        store_copy(0, d).start()
    for a in range(3):
        for d in range(4):
            store_copy(a, d).wait()
    for d in (1, 2, 3):
        x_copy(d).wait_send()
        branch_copy(d).wait_send()
        for a in range(3):
            for h in range(2):
                part_copy(a, d, h).wait_send()
    for d in (1, 2):
        for a in range(3):
            for h in range(2):
                spread_copy(a, d, h).wait_send()
            onward_copy(a, d).wait_send()

    @pl.when(is_top)
    def _():
        for d in (1, 2, 3):
            dy_copy(d).wait_send()
        for d in range(4):
            pass_copy(d).wait_send()


def update_kernel(x_ref, dy_ref, packed_ref, gate_out, up_out, down_out):
    for left, right, out in (
        (x_ref[...], packed_ref[1], gate_out),
        (x_ref[...], packed_ref[2], up_out),
        (packed_ref[0], dy_ref[...], down_out),
    ):
        out[...] = lax.dot_general(left, right, CONTRACT_ROWS, preferred_element_type=jnp.float32)


def weight_updates(x_whole, dy_whole, packed):
    rows, width = x_whole.shape
    hidden_width = packed.shape[2]
    tile = next(t for t in (512, 256, 128) if hidden_width % t == 0)
    f32 = jnp.float32
    whole = pl.BlockSpec((rows, width), lambda j: (0, 0))
    wide = pl.BlockSpec((width, tile), lambda j: (0, j))
    return pl.pallas_call(
        update_kernel,
        grid=(hidden_width // tile,),
        out_shape=(
            jax.ShapeDtypeStruct((width, hidden_width), f32),
            jax.ShapeDtypeStruct((width, hidden_width), f32),
            jax.ShapeDtypeStruct((hidden_width, width), f32),
        ),
        in_specs=[whole, whole, pl.BlockSpec((3, rows, tile), lambda j: (0, 0, j))],
        out_specs=(wide, wide, pl.BlockSpec((tile, width), lambda j: (j, 0))),
        compiler_params=pltpu.CompilerParams(vmem_limit_bytes=60 * 2**20),
    )(x_whole, dy_whole, packed)


def fast_shards(section_inputs, out_grad, gate_weight, up_weight, down_weight):
    panels = section_inputs[0]
    micro, local, width = panels.shape
    group = micro * local
    held = (local, micro, width)
    rows = group * lax.axis_size("col")
    hidden_width = gate_weight.shape[2]
    piece = hidden_width // lax.axis_size("row")
    vmem = pl.BlockSpec(memory_space=pltpu.VMEM)
    anywhere = pl.BlockSpec(memory_space=pl.ANY)
    bf16, f32 = jnp.bfloat16, jnp.float32
    dma = pltpu.SemaphoreType.DMA
    grad, x_whole, dy_whole, packed = pl.pallas_call(
        relay_kernel,
        out_shape=(
            jax.ShapeDtypeStruct(held, bf16),
            jax.ShapeDtypeStruct((rows, width), bf16),
            jax.ShapeDtypeStruct((rows, width), bf16),
            jax.ShapeDtypeStruct((3, rows, hidden_width), bf16),
        ),
        in_specs=[vmem, vmem, anywhere, anywhere, anywhere],
        out_specs=(vmem, vmem, vmem, anywhere),
        scratch_shapes=[
            pltpu.VMEM((4, width, piece), bf16),
            pltpu.VMEM((4, width, piece), bf16),
            pltpu.VMEM((4, piece, width), bf16),
            pltpu.VMEM((4, *held), bf16),
            pltpu.VMEM((4, *held), bf16),
            pltpu.VMEM((3, 4, rows, piece), bf16),
            pltpu.VMEM((3, 4, rows, piece), bf16),
            pltpu.VMEM((3, 4, rows, piece), bf16),
            pltpu.VMEM((rows, piece), f32),
            pltpu.VMEM((rows, piece), f32),
            pltpu.VMEM((rows, width), f32),
            pltpu.VMEM((4, group, width), bf16),
            pltpu.VMEM((4, group, width), bf16),
            pltpu.VMEM(held, bf16),
            dma((3, 4)), dma((4,)), dma((4,)), dma((4,)), dma((4,)),
            *[dma((3, 4, 2))] * 4, dma((4,)), dma((4,)),
            dma((3, 4)), dma((3, 4)), dma((3, 4)), pltpu.SemaphoreType.REGULAR,
        ],
        compiler_params=pltpu.CompilerParams(collective_id=0, has_side_effects=True, vmem_limit_bytes=56 * 2**20),
    )(
        panels.transpose(1, 0, 2), out_grad.transpose(1, 0, 2),
        gate_weight[0], up_weight[0], down_weight[0],
    )
    grads = weight_updates(x_whole, dy_whole, packed)
    grad = grad.transpose(1, 0, 2)
    return (grad[None], *(g[None] for g in grads))


def fits_kernel(mesh, gate_weight, section_inputs):
    sizes = mesh.shape
    if (sizes["section"], sizes["row"], sizes["col"]) != (2, 4, 4):
        return False
    piece = gate_weight.shape[2] // (sizes["row"] * sizes["col"])
    local = section_inputs.shape[1] * section_inputs.shape[2] // sizes["col"]
    return piece % 128 == 0 and local % 8 == 0 and (local * sizes["col"]) % 32 == 0


def solution(mesh):
    specs = dict(
        mesh=mesh,
        in_specs=(
            P("section", None, "col", "row"),
            P(None, "col", "row"),
            P("section", "row", "col"),
            P("section", "row", "col"),
            P("section", "col", "row"),
        ),
        out_specs=(
            P("section", None, "col", "row"),
            P("section", "row", "col"),
            P("section", "row", "col"),
            P("section", "col", "row"),
        ),
        check_vma=False,
    )

    def run(section_inputs, out_grad, gate_weight, up_weight, down_weight):
        body = fast_shards if fits_kernel(mesh, gate_weight, section_inputs) else shards
        return jax.shard_map(body, **specs)(section_inputs, out_grad, gate_weight, up_weight, down_weight)

    return run
```
